32 devices in a mesh: lon: 2 (over x), lat: 4 (over y, core), mem: 4 (over z).
Axes of the slice: x: 2, y: 2, z: 4, core: 2. Of those that a mesh axis runs over, the one named last changes fastest.
Arguments:
- anomalies: bfloat16 [32, 4, 128, 512], P('mem', None, 'lon', 'lat'), may hold values from -6 to 6
- spread: float32 [4, 128, 512], P(None, 'lon', 'lat'), may hold values from 0.5 to 2
- obs_index: int32 [2, 4, 2048], P('lon', 'lat'), may hold values from 0 to 32767
- innovation: float32 [2, 4, 2048], P('lon', 'lat'), may hold values from -6 to 6
- obs_weight: float32 [2, 4, 2048], P('lon', 'lat'), may hold values from 0.5 to 8
- band_width: int32 [2, 4], replicated, may hold values from 6 to 12, as said below
Outputs:
- control_ens: float32 [32, 4, 128, 512], P('mem', None, 'lon', 'lat')
- control_static: float32 [4, 128, 512], P(None, 'lon', 'lat')
The draws below stay inside these ranges and needn't reach their ends.
Inputs may be any that keep to these rules, and one draw needn't show every extreme that they name: `obs_index`: A cell of the tile's 4 x 64 x 128 block, flattened with latitude fastest. `band_width`: in each of the two rows some level has exactly 12.
All inputs are finite; a program needn't handle non-finite values.
Results may differ from the reference program's by a relative error of at most 0.0003.
Values may be sent and summed in bfloat16 or wider, within the bound.
A program may use at most 64 MiB of HBM per device.

```python
import math
import jax
import jax.numpy as jnp
from jax import lax

LON_DEV = 64
LAT_DEV = 128
LEVELS = 4
OBS_DEV = 2048
BAND = 12
ITERS = 2
MEMBERS = 32
NLON = 128
NLAT = 512
N_LON = 2
N_LAT = 4


def draw_band_width(key, part):
    lower = jax.random.randint(jax.random.fold_in(key, 11), (2, LEVELS), BAND // 2, BAND + 1)
    widest = jax.random.randint(jax.random.fold_in(key, 12), (2, 1), 0, LEVELS)
    level_iota = jnp.arange(LEVELS, dtype=jnp.int32)[None, :]
    return jnp.where(level_iota == widest, BAND, lower).astype(jnp.int32)


def with_ends(values, rng, least, largest):
    shape = values.shape
    index_at = [jax.random.randint(jax.random.fold_in(rng, axis), (), 0, shape[axis]) for axis in range(len(shape))]
    values = values.at[tuple(index_at)].set(least)
    longest = shape.index(max(shape))
    index_at[longest] = (index_at[longest] + 1) % shape[longest]
    return values.at[tuple(index_at)].set(largest)


def shard_levels(stream_key, dims, pieces, smallest, high):
    def one(position, blocks):
        draws = jax.random.uniform(jax.random.fold_in(jax.random.fold_in(stream_key, 6), position), (blocks,), jnp.float32, smallest / len(pieces), high / len(pieces))
        return jnp.repeat(jnp.exp(draws), dims[position] // blocks).reshape((-1,) + (1,) * (len(dims) - position - 1))

    loudness = one(*pieces[0])
    for cut in pieces[1:]:
        loudness = loudness * one(*cut)
    return loudness


def noise(key, dims, scale, reach, split=(), held_as=jnp.bfloat16):
    drawn = jax.random.normal(key, dims, jnp.float32) * scale
    if len(split) > 0:
        drawn = shard_levels(key, dims, split, -0.22, 0.18) * drawn
    return jnp.clip(drawn, min=-reach, max=reach).astype(held_as)


def setup_inputs(seed: int = 0) -> dict:
    streams_of = jax.random.split(jax.random.key(seed), 7)
    return {
        "anomalies": noise(streams_of[0], (MEMBERS, LEVELS, NLON, NLAT), 1.0, 6.0, ((0, 4), (2, 2), (3, 4))),
        "spread": jnp.clip(jnp.exp(math.log(2.0) - 1.3862944 * jax.random.uniform(streams_of[1], (LEVELS, NLON, NLAT), jnp.float32) ** shard_levels(streams_of[1], (LEVELS, NLON, NLAT), ((1, 2), (2, 4)), -0.2, 0.2)), 0.5, 2.0),
        "obs_index": with_ends(jax.random.randint(streams_of[2], (N_LON, N_LAT, OBS_DEV), 0, LEVELS * LON_DEV * LAT_DEV), jax.random.fold_in(streams_of[2], 1), 0, (LEVELS * LON_DEV * LAT_DEV) - 1).astype(jnp.int32),
        "innovation": noise(streams_of[3], (N_LON, N_LAT, OBS_DEV), 1.0, 6.0, ((0, 2), (1, 4)), jnp.float32),
        "obs_weight": jnp.clip(jnp.exp(math.log(8.0) - 2.7725887 * jax.random.uniform(streams_of[4], (N_LON, N_LAT, OBS_DEV), jnp.float32) ** shard_levels(streams_of[4], (N_LON, N_LAT, OBS_DEV), ((0, 2), (1, 4)), -0.2, 0.2)), 0.5, 8.0),
        "band_width": draw_band_width(jax.random.fold_in(streams_of[6], 71), 0),
    }


hybrid_ens = 0.75
hybrid_static = 0.25

def band_table(band_width):
    offsets = jnp.arange(-BAND, BAND + 1).astype(jnp.float32)
    widths = band_width.astype(jnp.float32)[..., None]
    shape_raw = jnp.exp(-0.5 * (offsets / (0.5 * widths)) ** 2)
    shape_raw = jnp.where(jnp.abs(offsets) <= widths, shape_raw, 0.0)
    return shape_raw / lax.optimization_barrier(jnp.sum(shape_raw, axis=-1, keepdims=True))

def localize(field, weights_lon, weights_lat):
    lon_smooth = jnp.zeros_like(field)
    for shift in range(2 * BAND + 1):
        lon_smooth = lon_smooth + weights_lon[:, shift][:, None, None] * jnp.roll(field, BAND - shift, axis=1)
    padded = jnp.pad(lon_smooth, ((0, 0), (0, 0), (BAND, BAND)))
    result = jnp.zeros_like(field)
    for shift in range(2 * BAND + 1):
        result = result + weights_lat[:, shift][:, None, None] * padded[:, :, shift:shift + NLAT]
    return result

def reference(anomalies, spread, obs_index, innovation, obs_weight, band_width):
    band_weights = band_table(band_width)
    coef_ens = math.sqrt(hybrid_ens / MEMBERS)
    coef_static = math.sqrt(hybrid_static)

    def smooth(fields):
        return lax.map(lambda member_field: localize(member_field, band_weights[0], band_weights[1]), fields)
    plane_cells = LON_DEV * LAT_DEV
    obs_level = obs_index // plane_cells
    in_plane = obs_index % plane_cells
    tile_lon = jnp.arange(N_LON, dtype=jnp.int32)[:, None, None]
    tile_lat = jnp.arange(N_LAT, dtype=jnp.int32)[None, :, None]
    flat_index = ((obs_level * NLON + tile_lon * LON_DEV + in_plane // LAT_DEV) * NLAT + tile_lat * LAT_DEV + in_plane % LAT_DEV).reshape(-1).astype(jnp.int32)
    weights = obs_weight.reshape(-1)
    values = innovation.reshape(-1)
    cell_count = LEVELS * NLON * NLAT

    def scatter(obs_term):
        return jnp.zeros((cell_count,), jnp.float32).at[flat_index].add(obs_term).reshape(LEVELS, NLON, NLAT)

    def adjoint(gradient):
        products = jnp.concatenate([coef_ens * anomalies.astype(jnp.float32) * gradient[None], (coef_static * spread * gradient)[None]], axis=0)
        return smooth(products)

    def hessian(direction):
        localized = smooth(direction)
        combined = coef_ens * lax.optimization_barrier(jnp.sum(anomalies.astype(jnp.float32) * localized[:MEMBERS], axis=0)) + coef_static * spread * localized[MEMBERS]
        gradient = scatter(weights * combined.reshape(-1)[flat_index])
        return direction + adjoint(gradient)
    right_side = adjoint(scatter(weights * values))
    control = jnp.zeros_like(right_side)
    residual = right_side
    direction = right_side
    norm_now = jnp.sum(residual * residual)
    for iteration in range(ITERS):
        hess_image = hessian(direction)
        step_size = norm_now / jnp.sum(direction * hess_image)
        control = control + step_size * direction
        residual = residual - step_size * hess_image
        norm_next = jnp.sum(residual * residual)
        direction = residual + norm_next / norm_now * direction
        norm_now = norm_next
    return (control[:MEMBERS], control[MEMBERS])
```

```python
import functools
import math

import jax
import jax.numpy as jnp
from jax import lax
from jax.experimental import pallas as pl
from jax.experimental.pallas import tpu as pltpu
from jax.sharding import PartitionSpec as P

BAND = 12
RIM = 2 * BAND

hybrid_ens = 0.75
hybrid_static = 0.25

MESH = pl.DeviceIdType.MESH
VMEM = pl.BlockSpec(memory_space=pltpu.VMEM)
F32 = jnp.float32
BF16 = jnp.bfloat16


def split2(x):
    hi = x.astype(BF16)
    return hi, (x - hi.astype(F32)).astype(BF16)


def dot3(left, right):
    lh, ll = left
    rh, rl = right
    d = functools.partial(jnp.dot, preferred_element_type=F32)
    return d(lh, rh) + (d(ll, rh) + d(lh, rl))


def exchange(axis, to_low, to_high, cid):
    count = len(to_low)
    n = lax.axis_size(axis)

    def kernel(*refs):
        low_in, high_in = refs[:count], refs[count : 2 * count]
        from_low, from_high = refs[2 * count : 3 * count], refs[3 * count : 4 * count]
        send, recv = refs[4 * count :]
        me = lax.axis_index(axis)
        low, high = lax.rem(me + n - 1, n), lax.rem(me + 1, n)
        barrier = pltpu.get_barrier_semaphore()
        for other in (low, high):
            pl.semaphore_signal(barrier, inc=1, device_id={axis: other}, device_id_type=MESH)
        pl.semaphore_wait(barrier, 2)
        copies = []
        for i in range(count):
            for side, (src, dst, other) in enumerate(
                ((low_in[i], from_high[i], low), (high_in[i], from_low[i], high))
            ):
                copy = pltpu.make_async_remote_copy(
                    src_ref=src,
                    dst_ref=dst,
                    send_sem=send.at[2 * i + side],
                    recv_sem=recv.at[2 * i + side],
                    device_id={axis: other},
                    device_id_type=MESH,
                )
                copy.start()
                copies.append(copy)
        for copy in copies:
            copy.wait()

    shapes = [jax.ShapeDtypeStruct(a.shape, a.dtype) for a in (*to_high, *to_low)]
    out = pl.pallas_call(
        kernel,
        out_shape=shapes,
        in_specs=[VMEM] * (2 * count),
        out_specs=[VMEM] * (2 * count),
        scratch_shapes=[
            pltpu.SemaphoreType.DMA((2 * count,)),
            pltpu.SemaphoreType.DMA((2 * count,)),
        ],
        compiler_params=pltpu.CompilerParams(collective_id=cid, has_side_effects=True),
    )(*to_low, *to_high)
    return out[:count], out[count:]


def mem_sum(part, cid, gather):
    axis = "mem"
    n = lax.axis_size(axis)
    rows, lanes = part.shape
    chunk = rows // n

    def kernel(x_ref, out_ref, slots, send, recv, send2, recv2):
        me = lax.axis_index(axis)
        barrier = pltpu.get_barrier_semaphore()
        for j in range(1, n):
            pl.semaphore_signal(
                barrier, inc=1, device_id={axis: lax.rem(me + j, n)}, device_id_type=MESH
            )
        pl.semaphore_wait(barrier, n - 1)

        def piece(owner):
            return pl.ds(pl.multiple_of(owner * chunk, chunk), chunk)

        copies = []
        for j in range(1, n):
            peer = lax.rem(me + j, n)
            copy = pltpu.make_async_remote_copy(
                src_ref=x_ref.at[piece(peer)],
                dst_ref=slots.at[j],
                send_sem=send.at[j],
                recv_sem=recv.at[j],
                device_id={axis: peer},
                device_id_type=MESH,
            )
            copy.start()
            copies.append(copy)
        total = x_ref[piece(me), :]
        for j, copy in enumerate(copies):
            copy.wait_recv()
            total = total + slots[j + 1]
        if gather:
            out_ref[piece(me), :] = total
            back = []
            for j in range(1, n):
                peer = lax.rem(me + j, n)
                copy = pltpu.make_async_remote_copy(
                    src_ref=out_ref.at[piece(me)],
                    dst_ref=out_ref.at[piece(me)],
                    send_sem=send2.at[j],
                    recv_sem=recv2.at[j],
                    device_id={axis: peer},
                    device_id_type=MESH,
                )
                copy.start()
                back.append(copy)
            for copy in back:
                copy.wait()
        else:
            out_ref[...] = total
        for copy in copies:
            copy.wait_send()

    return pl.pallas_call(
        kernel,
        out_shape=jax.ShapeDtypeStruct((rows if gather else chunk, lanes), F32),
        in_specs=[VMEM],
        out_specs=VMEM,
        scratch_shapes=[pltpu.VMEM((n, chunk, lanes), F32)]
        + [pltpu.SemaphoreType.DMA((n,)) for _ in range(4)],
        compiler_params=pltpu.CompilerParams(collective_id=cid, has_side_effects=True),
    )(part)


def all_sum(block, cid):
    axes = ("lon", "lat", "mem")
    sizes = [lax.axis_size(a) for a in axes]
    total = math.prod(sizes)

    def kernel(x_ref, out_ref, slots, send, recv):
        mine = [lax.axis_index(a) for a in axes]

        def shifted(step):
            parts, rest = [], step
            for size in reversed(sizes):
                parts.append(rest % size)
                rest //= size
            return tuple(
                lax.rem(m + s, size) for m, s, size in zip(mine, reversed(parts), sizes)
            )

        barrier = pltpu.get_barrier_semaphore()
        for step in range(1, total):
            pl.semaphore_signal(barrier, inc=1, device_id=shifted(step), device_id_type=MESH)
        pl.semaphore_wait(barrier, total - 1)
        copies = []
        for step in range(1, total):
            copy = pltpu.make_async_remote_copy(
                src_ref=x_ref,
                dst_ref=slots.at[step],
                send_sem=send.at[step],
                recv_sem=recv.at[step],
                device_id=shifted(step),
                device_id_type=MESH,
            )
            copy.start()
            copies.append(copy)
        slots[0] = x_ref[...]
        for copy in copies:
            copy.wait()
        out_ref[...] = jnp.sum(slots[...], axis=0)

    return pl.pallas_call(
        kernel,
        out_shape=jax.ShapeDtypeStruct(block.shape, F32),
        in_specs=[VMEM],
        out_specs=VMEM,
        scratch_shapes=[
            pltpu.VMEM((total, *block.shape), F32),
            pltpu.SemaphoreType.DMA((total,)),
            pltpu.SemaphoreType.DMA((total,)),
        ],
        compiler_params=pltpu.CompilerParams(collective_id=cid, has_side_effects=True),
    )(block)


def scatter_obs(index, weight, innovation, rows, lanes):
    def kernel(i_ref, w_ref, v_ref, d_ref, b_ref):
        idx = i_ref[...]
        w = w_ref[...]
        n = idx.shape[1]
        row, lane = idx // lanes, idx % lanes
        at_row = (lax.broadcasted_iota(jnp.int32, (rows, n), 0) == row).astype(F32).astype(BF16)
        at_lane = lax.broadcasted_iota(jnp.int32, (lanes, n), 0) == lane
        for val, out in ((w, d_ref), (w * v_ref[...], b_ref)):
            acc = None
            for _ in range(3):
                part = val.astype(BF16).astype(F32)
                val = val - part
                spread_out = jnp.where(at_lane, part, 0.0).astype(BF16)
                term = lax.dot_general(
                    at_row, spread_out, (((1,), (1,)), ((), ())), preferred_element_type=F32
                )
                acc = term if acc is None else acc + term
            out[...] = acc

    return pl.pallas_call(
        kernel,
        out_shape=[jax.ShapeDtypeStruct((rows, lanes), F32)] * 2,
        in_specs=[VMEM] * 3,
        out_specs=[VMEM] * 2,
    )(index, weight, innovation)


def smooth_level(fc, fr, yc, yr, mc, mr, ml):
    fields = fc.shape[0]
    ext, lanes = yc.shape
    xc = (fc[...] * yc[None]).reshape(fields * ext, lanes)
    xr = (fr[...] * yr[None]).reshape(fields * ext, yr.shape[1])
    t = dot3(split2(xc), split2(mc)) + dot3(split2(xr), split2(mr))
    th, tl = split2(t)
    lon = split2(ml)
    return [
        dot3(lon, (th[f * ext : (f + 1) * ext], tl[f * ext : (f + 1) * ext]))
        for f in range(fields)
    ]


def apply_cov(fc, fr, yc, yr, mats, lon_cells, mem_count):
    levels, fields, ext, lanes = fc.shape
    mc, mr, ml = mats

    def kernel(fc_ref, fr_ref, yc_ref, yr_ref, mc_ref, mr_ref, ml_ref, out_ref):
        smoothed = smooth_level(
            fc_ref.at[0], fr_ref, yc_ref[0], yr_ref[...], mc_ref[0], mr_ref[0], ml_ref[0]
        )
        acc = fc_ref[0, fields - 1, :lon_cells, :] * smoothed[-1] * (1.0 / mem_count)
        for f in range(fields - 1):
            acc = acc + fc_ref[0, f, :lon_cells, :] * smoothed[f]
        out_ref[0] = acc

    def level(*shape):
        return pl.BlockSpec((1, *shape), lambda l: (l,) + (0,) * len(shape))

    return pl.pallas_call(
        kernel,
        grid=(levels,),
        out_shape=jax.ShapeDtypeStruct((levels, lon_cells, lanes), F32),
        in_specs=[
            level(*fc.shape[1:]),
            VMEM,
            level(*yc.shape[1:]),
            VMEM,
            level(*mc.shape[1:]),
            level(*mr.shape[1:]),
            level(*ml.shape[1:]),
        ],
        out_specs=level(lon_cells, lanes),
    )(fc, fr, yc, yr, mc, mr, ml)


def apply_adjoint(fc, fr, yc, yr, mats, lon_cells):
    levels, fields, ext, lanes = fc.shape
    mc, mr, ml = mats

    def kernel(fc_ref, fr_ref, yc_ref, yr_ref, mc_ref, mr_ref, ml_ref, ens_ref, static_ref):
        smoothed = smooth_level(
            fc_ref.at[0], fr_ref, yc_ref[0], yr_ref[...], mc_ref[0], mr_ref[0], ml_ref[0]
        )
        for f in range(fields - 1):
            ens_ref[f, 0] = smoothed[f]
        static_ref[0] = smoothed[-1]

    def level(*shape):
        return pl.BlockSpec((1, *shape), lambda l: (l,) + (0,) * len(shape))

    return pl.pallas_call(
        kernel,
        grid=(levels,),
        out_shape=[
            jax.ShapeDtypeStruct((fields - 1, levels, lon_cells, lanes), F32),
            jax.ShapeDtypeStruct((levels, lon_cells, lanes), F32),
        ],
        in_specs=[
            level(*fc.shape[1:]),
            VMEM,
            level(*yc.shape[1:]),
            VMEM,
            level(*mc.shape[1:]),
            level(*mr.shape[1:]),
            level(*ml.shape[1:]),
        ],
        out_specs=[
            pl.BlockSpec((fields - 1, 1, lon_cells, lanes), lambda l: (0, l, 0, 0)),
            level(lon_cells, lanes),
        ],
    )(fc, fr, yc, yr, mc, mr, ml)


def pack_lat(x, side):
    lanes = x.shape[-1]
    cut = slice(0, RIM) if side == 0 else slice(lanes - RIM, lanes)
    return jnp.concatenate([x[..., l, :, cut] for l in range(x.shape[-3])], axis=-1)


def rows_of(x, side):
    rows = x.shape[-2]
    return x[..., :RIM, :] if side == 0 else x[..., rows - RIM :, :]


def extend(arrays, cids):
    lat_n = lax.axis_size("lat")
    at = lax.axis_index("lat")
    lows, highs = exchange(
        "lat", [pack_lat(x, 0) for x in arrays], [pack_lat(x, 1) for x in arrays], cids[0]
    )
    rims = []
    for low, high in zip(lows, highs):
        low = jnp.where(at > 0, low, jnp.zeros_like(low))
        high = jnp.where(at < lat_n - 1, high, jnp.zeros_like(high))
        rims.append((low, high))

    def lon_pack(x, rim, side):
        body = rows_of(x, side)
        body = body.reshape(*x.shape[:-3], x.shape[-3] * RIM, x.shape[-1])
        edge = jnp.concatenate([rows_of(rim[0], side), rows_of(rim[1], side)], axis=-2)
        return body, edge

    to_low, to_high = [], []
    for x, rim in zip(arrays, rims):
        to_low.extend(lon_pack(x, rim, 0))
        to_high.extend(lon_pack(x, rim, 1))
    from_low, from_high = exchange("lon", to_low, to_high, cids[1])
    out = []
    for i, (x, rim) in enumerate(zip(arrays, rims)):
        shape = (*x.shape[:-2], RIM, x.shape[-1])
        center = jnp.concatenate(
            [x, from_low[2 * i].reshape(shape), from_high[2 * i].reshape(shape)], axis=-2
        )
        sides = []
        for s in range(2):
            cut = slice(s * RIM, (s + 1) * RIM)
            sides.append(
                jnp.concatenate(
                    [rim[s], from_low[2 * i + 1][..., cut, :], from_high[2 * i + 1][..., cut, :]],
                    axis=-2,
                )
            )
        out.append((center, jnp.concatenate(sides, axis=-1)))
    return out


def band_weight(widths, offset):
    w = widths.astype(F32)
    taps = jnp.arange(-BAND, BAND + 1).astype(F32)

    def shape_of(o, width):
        raw = jnp.exp(-0.5 * (o / (0.5 * width)) ** 2)
        return jnp.where(jnp.abs(o) <= width, raw, 0.0)

    norm = jnp.sum(shape_of(taps[None, :], w[:, None]), axis=1)
    return shape_of(offset.astype(F32)[None], w[:, None, None]) / norm[:, None, None]


def matrices(band_width, lon_cells, lat_cells):
    levels = band_width.shape[1]
    mm = functools.partial(jnp.einsum, precision=lax.Precision.HIGHEST)
    own = jnp.arange(lon_cells)
    ext = jnp.concatenate([own, jnp.arange(-RIM, 0), lon_cells + jnp.arange(RIM)])
    mid = jnp.arange(-BAND, lon_cells + BAND)
    first = band_weight(band_width[0], own[:, None] - mid[None, :])
    second = band_weight(band_width[0], mid[:, None] - ext[None, :])
    lon_two = mm("lim,lmj->lij", first, second)
    lon_one = band_weight(band_width[0], own[:, None] - ext[None, :])
    own = jnp.arange(lat_cells)
    ext = jnp.concatenate([own, jnp.arange(-RIM, 0), lat_cells + jnp.arange(RIM)])
    mid = jnp.arange(-BAND, lat_cells + BAND)
    place = lax.axis_index("lat") * lat_cells + mid
    inside = (place >= 0) & (place < lat_cells * lax.axis_size("lat"))
    first = band_weight(band_width[1], ext[:, None] - mid[None, :])
    second = band_weight(band_width[1], mid[:, None] - own[None, :])
    second = jnp.where(inside[None, :, None], second, 0.0)
    lat_two = mm("lim,lmj->lij", first, second)
    lat_one = band_weight(band_width[1], ext[:, None] - own[None, :])

    def halves(lat):
        sel = jnp.eye(levels, dtype=F32)
        rims = []
        for s in range(2):
            part = lat[:, lat_cells + s * RIM : lat_cells + (s + 1) * RIM]
            rims.append(
                (sel[:, :, None, None] * part[:, None]).reshape(levels, levels * RIM, lat_cells)
            )
        return lat[:, :lat_cells], jnp.concatenate(rims, axis=1)

    return (*halves(lat_two), lon_two), (*halves(lat_one), lon_one)


def per_device(anomalies, spread, obs_index, innovation, obs_weight, band_width):
    members = anomalies.shape[0]
    levels, lon_cells, lat_cells = spread.shape
    mem_count = lax.axis_size("mem")
    coef_ens = math.sqrt(hybrid_ens / (members * mem_count))
    coef_static = math.sqrt(hybrid_static)
    rows = levels * lon_cells
    field = (levels, lon_cells, lat_cells)

    diag, rhs = scatter_obs(
        obs_index.reshape(1, -1), obs_weight.reshape(1, -1), innovation.reshape(1, -1), rows, lat_cells
    )
    two, one = matrices(band_width, lon_cells, lat_cells)

    (ac, ar), (sc, sr), (bc, br) = extend([anomalies, spread, rhs.reshape(field)], (0, 1))
    ac = jnp.swapaxes(ac, 0, 1).astype(F32)
    fc = jnp.concatenate([coef_ens * ac, coef_static * sc[:, None]], axis=1)
    fr = jnp.concatenate([coef_ens * ar.astype(F32), coef_static * sr[None]], axis=0)

    cov_b = mem_sum(
        apply_cov(fc, fr, bc, br, two, lon_cells, mem_count).reshape(rows, lat_cells), 2, True
    )
    image = rhs + diag * cov_b
    scale = 1.0 / mem_count

    def dots(left, right):
        a = jnp.sum(left.reshape(-1, 8, lat_cells), axis=0)
        b = jnp.sum(right.reshape(-1, 8, lat_cells), axis=0)
        a, b = jnp.sum(a, axis=0, keepdims=True), jnp.sum(b, axis=0, keepdims=True)
        pad = jnp.zeros((6, lat_cells), F32)
        total = jnp.sum(all_sum(jnp.concatenate([a, b, pad], axis=0), 3), axis=1)
        return total[0], total[1]

    norm0, curve0 = dots(scale * (rhs * cov_b), scale * (cov_b * image))
    alpha0 = norm0 / curve0
    ((qc, qr),) = extend([image.reshape(field)], (4, 5))
    cov_q = mem_sum(
        apply_cov(fc, fr, qc, qr, two, lon_cells, mem_count).reshape(rows, lat_cells), 6, False
    )
    chunk = rows // mem_count
    start = lax.axis_index("mem") * chunk

    def mine(x):
        return lax.dynamic_slice_in_dim(x, start, chunk, axis=0)

    resid = mine(rhs) - alpha0 * mine(image)
    cov_r = mine(cov_b) - alpha0 * cov_q
    norm1, curve1 = dots(resid * cov_r, cov_r * (resid + mine(diag) * cov_r))
    beta = norm1 / norm0
    alpha1 = norm1 / (curve1 - beta * norm1 / alpha0)
    cc = alpha0 * bc + alpha1 * ((bc - alpha0 * qc) + beta * bc)
    cr = alpha0 * br + alpha1 * ((br - alpha0 * qr) + beta * br)
    ens, static = apply_adjoint(fc, fr, cc, cr, one, lon_cells)
    return ens, static


def solution(mesh):
    return jax.shard_map(
        per_device,
        mesh=mesh,
        in_specs=(
            P("mem", None, "lon", "lat"),
            P(None, "lon", "lat"),
            P("lon", "lat", None),
            P("lon", "lat", None),
            P("lon", "lat", None),
            P(),
        ),
        out_specs=(P("mem", None, "lon", "lat"), P(None, "lon", "lat")),
        check_vma=False,
    )
```

```python
import functools
import math

import jax
import jax.numpy as jnp
from jax import lax
from jax.experimental import pallas as pl
from jax.experimental.pallas import tpu as pltpu
from jax.sharding import PartitionSpec as P

BAND = 12
RIM = 2 * BAND

hybrid_ens = 0.75
hybrid_static = 0.25

MESH = pl.DeviceIdType.MESH
VMEM = pl.BlockSpec(memory_space=pltpu.VMEM)
F32 = jnp.float32
BF16 = jnp.bfloat16


def split2(x):
    hi = x.astype(BF16)
    return hi, (x - hi.astype(F32)).astype(BF16)


def dot3(left, right):
    lh, ll = left
    rh, rl = right
    d = functools.partial(jnp.dot, preferred_element_type=F32)
    return d(lh, rh) + (d(ll, rh) + d(lh, rl))


AXES = ("lon", "lat", "mem")


def fused(a_ref, s_ref, i_ref, w_ref, v_ref, bw_ref, ens_ref, static_ref, *scratch, dims):
    members, levels, lon_cells, lat_cells, sizes = dims
    (fc, fr, bc, br, qc, qr, send_al, send_ah, recv_al, recv_ah, pack_l, pack_h, recv_pl, recv_ph,
     fpack, xrh, xrl, two_c, two_r, two_l, one_c, one_r, one_l, bflat, dflat, cov, part,
     slots, slots2, dslots, dsend, send, recv, csend, crecv, dsems, drems) = scratch
    lon_n, lat_n, mem_n = sizes
    total = lon_n * lat_n * mem_n
    fields = members + 1
    ext = lon_cells + 2 * RIM
    rows = levels * lon_cells
    chunk = rows // mem_n
    coef_ens = math.sqrt(hybrid_ens / (members * mem_n))
    coef_static = math.sqrt(hybrid_static)
    mine = [lax.axis_index(a) for a in AXES]
    lat_at, me = mine[1], mine[2]
    has_low, has_high = lat_at > 0, lat_at < lat_n - 1

    def shifted(step):
        parts, rest = [], step
        for size in reversed(sizes):
            parts.append(rest % size)
            rest //= size
        return tuple(lax.rem(m + s, size) for m, s, size in zip(mine, reversed(parts), sizes))

    barrier = pltpu.get_barrier_semaphore()
    for step in range(1, total):
        pl.semaphore_signal(barrier, inc=1, device_id=shifted(step), device_id_type=MESH)

    used = [0]

    def remote(src, dst, where):
        k = used[0]
        used[0] += 1
        return pltpu.make_async_remote_copy(
            src_ref=src, dst_ref=dst, send_sem=send.at[k], recv_sem=recv.at[k],
            device_id=where, device_id_type=MESH,
        )

    lon_low = {"lon": lax.rem(mine[0] + lon_n - 1, lon_n)}
    lon_high = {"lon": lax.rem(mine[0] + 1, lon_n)}
    lat_low = {"lat": lax.rem(lat_at + lat_n - 1, lat_n)}
    lat_high = {"lat": lax.rem(lat_at + 1, lat_n)}
    own = pl.ds(0, lon_cells)
    rim = pl.ds(lon_cells, 2 * RIM)
    low_rows = pl.ds(lon_cells, RIM)
    high_rows = pl.ds(lon_cells + RIM, RIM)
    first_rows = pl.ds(0, RIM)
    last_rows = pl.ds(lon_cells - RIM, RIM)
    low_lanes = pl.ds(0, lat_cells)
    high_lanes = pl.ds(lat_cells, lat_cells)

    def lon_start(copies):
        for c in copies:
            c.start()

    def lon_wait(copies):
        for c in copies:
            c.wait()

    class Lat:
        def __init__(self, low_src, high_src, from_low, from_high):
            self.to_low = remote(low_src, from_high, lat_low)
            self.to_high = remote(high_src, from_low, lat_high)

        def start(self):
            pl.when(has_low)(self.to_low.start)
            pl.when(has_high)(self.to_high.start)

        def wait(self):
            pl.when(has_low)(self.to_low.wait_send)
            pl.when(has_high)(self.to_high.wait_send)
            pl.when(has_high)(self.to_low.wait_recv)
            pl.when(has_low)(self.to_high.wait_recv)

    def lane_pack(read, count):
        lane = lax.broadcasted_iota(jnp.int32, (count, lat_cells), 1)
        low = jnp.zeros((count, lat_cells), F32)
        high = low
        for l in range(levels):
            x = read(l)
            here = (lane >= l * RIM) & (lane < (l + 1) * RIM)
            low = jnp.where(here, pltpu.roll(x, (l * RIM) % lat_cells, 1), low)
            high = jnp.where(here, pltpu.roll(x, ((l + 1) * RIM) % lat_cells, 1), high)
        return low, high

    def zero_edges(ref, lead=()):
        @pl.when(jnp.logical_not(has_low))
        def _():
            ref[(*lead, slice(None), low_lanes)] = jnp.zeros((ext, lat_cells), F32)

        @pl.when(jnp.logical_not(has_high))
        def _():
            ref[(*lead, slice(None), high_lanes)] = jnp.zeros((ext, lat_cells), F32)

    def load_member(m, _):
        lows, highs = [], []
        for l in range(levels):
            x = a_ref[m, l].astype(F32)
            fc[l, m, :lon_cells, :] = x
            lows.append(x[:RIM])
            highs.append(x[lon_cells - RIM :])
        send_al[m] = jnp.concatenate(lows, axis=0).astype(BF16)
        send_ah[m] = jnp.concatenate(highs, axis=0).astype(BF16)
        return 0

    lax.fori_loop(0, members, load_member, 0)
    for l in range(levels):
        fc[l, members, :lon_cells, :] = s_ref[l]

    def pack_member(span, count):
        def go(m, _):
            low, high = lane_pack(lambda l: fc[l, m, span, :], count)
            pack_l[m, span, :] = low.astype(BF16)
            pack_h[m, span, :] = high.astype(BF16)
            return 0

        lax.fori_loop(0, members, go, 0)

    def lon_field(ref, lead):
        at = lambda span: ref.at[(slice(None), *lead, span, slice(None))]
        return [
            remote(at(first_rows), at(high_rows), lon_low),
            remote(at(last_rows), at(low_rows), lon_high),
        ]

    def lat_field(slot, dst, lead, span):
        at = lambda lanes: dst.at[(*lead, span, lanes)]
        return Lat(
            fpack.at[slot, 0, span, :], fpack.at[slot, 1, span, :], at(low_lanes), at(high_lanes)
        )

    def fill_pack(slot, read, span, count):
        low, high = lane_pack(lambda l: read(l, span), count)
        fpack[slot, 0, span, :] = low
        fpack[slot, 1, span, :] = high

    read_s = lambda l, span: fc[l, members, span, :]
    read_b = lambda l, span: bc[l, span, :]
    read_q = lambda l, span: qc[l, span, :]

    pl.semaphore_wait(barrier, total - 1)
    lon_a = [remote(send_al, recv_ah, lon_low), remote(send_ah, recv_al, lon_high)]
    lon_start(lon_a)
    lon_s = lon_field(fc, (members,))
    lon_start(lon_s)
    pack_member(own, lon_cells)
    lat_a = Lat(pack_l.at[:, own, :], pack_h.at[:, own, :], recv_pl.at[:, own, :], recv_ph.at[:, own, :])
    lat_a.start()

    idx, val_w = i_ref[...], w_ref[...]
    n_obs = idx.shape[1]
    row, lane = idx // lat_cells, idx % lat_cells
    at_row = (lax.broadcasted_iota(jnp.int32, (rows, n_obs), 0) == row).astype(F32).astype(BF16)
    at_lane = lax.broadcasted_iota(jnp.int32, (lat_cells, n_obs), 0) == lane
    for val, out in ((val_w, dflat), (val_w * v_ref[...], bflat)):
        acc = None
        for _ in range(3):
            piece_val = val.astype(BF16).astype(F32)
            val = val - piece_val
            placed = jnp.where(at_lane, piece_val, 0.0).astype(BF16)
            term = lax.dot_general(
                at_row, placed, (((1,), (1,)), ((), ())), preferred_element_type=F32
            )
            acc = term if acc is None else acc + term
        out[...] = acc
    for l in range(levels):
        bc[l, :lon_cells, :] = bflat[l * lon_cells : (l + 1) * lon_cells, :]
    lon_b = lon_field(bc, ())
    lon_start(lon_b)
    fill_pack(0, read_s, own, lon_cells)
    fill_pack(1, read_b, own, lon_cells)
    lat_sb = [lat_field(0, fr, (members,), own), lat_field(1, br, (), own)]
    for c in lat_sb:
        c.start()
    zero_edges(fr, (members,))
    zero_edges(br)
    zero_edges(qr)

    def iota(shape, dim):
        return lax.broadcasted_iota(jnp.int32, shape, dim)

    def ext_place(index, cells):
        return jnp.where(index < cells, index, jnp.where(index < cells + RIM, index - cells - RIM, index - RIM))

    def make_matrices(l, _):
        taps = (iota((8, 128), 1) - BAND).astype(F32)

        def weights(kind):
            width = bw_ref[kind, l].astype(F32) + jnp.zeros((1, 1), F32)

            def raw(o):
                return jnp.where(jnp.abs(o) <= width, jnp.exp(-0.5 * (o / (0.5 * width)) ** 2), 0.0)

            norm = jnp.sum(raw(taps)[:1], axis=1, keepdims=True)
            return lambda o: raw(o.astype(F32)) / norm

        def put(ref, where, value):
            hi, lo = split2(value)
            ref[(0, *where)] = hi
            ref[(1, *where)] = lo

        w = weights(0)
        mids = 128 * pl.cdiv(lon_cells + 2 * BAND, 128)
        near = w(iota((lon_cells, mids), 0) - (iota((lon_cells, mids), 1) - BAND))
        near = jnp.where(iota((lon_cells, mids), 1) < lon_cells + 2 * BAND, near, 0.0)
        far = w(iota((mids, ext), 0) - BAND - ext_place(iota((mids, ext), 1), lon_cells))
        put(two_l, (l,), dot3(split2(near), split2(far)))
        put(one_l, (l,), w(iota((lon_cells, ext), 0) - ext_place(iota((lon_cells, ext), 1), lon_cells)))

        w = weights(1)
        mids = 128 * pl.cdiv(lat_cells + 2 * BAND, 128)
        mid = iota((mids, lat_cells), 0) - BAND
        place = lat_at * lat_cells + mid
        keep = (place >= 0) & (place < lat_cells * lat_n) & (mid < lat_cells + BAND)
        back = split2(jnp.where(keep, w(mid - iota((mids, lat_cells), 1)), 0.0))
        out = iota((lat_cells, lat_cells), 1)
        here = iota((lat_cells, mids), 0) - (iota((lat_cells, mids), 1) - BAND)
        put(two_c, (l,), dot3(split2(w(here)), back))
        put(one_c, (l,), w(iota((lat_cells, lat_cells), 0) - out))
        columns = pl.ds(pl.multiple_of(l * lat_cells, lat_cells), lat_cells)
        for side in range(2):
            shift = -RIM if side == 0 else lat_cells
            span = pl.ds(side * lat_cells, lat_cells)

            def rim_at(shape):
                p = iota(shape, 0) - l * RIM
                return p + shift, (p >= 0) & (p < RIM)

            pos, ok = rim_at((lat_cells, mids))
            there = jnp.where(ok, w(pos - (iota((lat_cells, mids), 1) - BAND)), 0.0)
            put(two_r, (span, columns), dot3(split2(there), back))
            pos, ok = rim_at((lat_cells, lat_cells))
            put(one_r, (span, columns), jnp.where(ok, w(pos - out), 0.0))
        return 0

    lax.fori_loop(0, levels, make_matrices, 0)

    lon_wait(lon_a)

    def unpack_member(m, _):
        low, high = recv_al[m].astype(F32), recv_ah[m].astype(F32)
        for l in range(levels):
            fc[l, m, low_rows, :] = low[l * RIM : (l + 1) * RIM]
            fc[l, m, high_rows, :] = high[l * RIM : (l + 1) * RIM]
        return 0

    lax.fori_loop(0, members, unpack_member, 0)
    pack_member(rim, 2 * RIM)
    lat_a2 = Lat(pack_l.at[:, rim, :], pack_h.at[:, rim, :], recv_pl.at[:, rim, :], recv_ph.at[:, rim, :])
    lat_a2.start()
    lon_wait(lon_s)
    lon_wait(lon_b)
    fill_pack(0, read_s, rim, 2 * RIM)
    fill_pack(1, read_b, rim, 2 * RIM)
    lat_sb2 = [lat_field(0, fr, (members,), rim), lat_field(1, br, (), rim)]
    for c in lat_sb2:
        c.start()
    lat_a.wait()
    lat_a2.wait()
    for ref, keep, lanes in ((recv_pl, has_low, low_lanes), (recv_ph, has_high, high_lanes)):
        @pl.when(keep)
        def _():
            def go(m, _):
                fr[m, :, lanes] = ref[m].astype(F32)
                return 0

            lax.fori_loop(0, members, go, 0)

        @pl.when(jnp.logical_not(keep))
        def _():
            def go(m, _):
                fr[m, :, lanes] = jnp.zeros((ext, lat_cells), F32)
                return 0

            lax.fori_loop(0, members, go, 0)

    for c in lat_sb + lat_sb2:
        c.wait()

    def apply(yc, yr, c_mat, r_mat, l_mat, finish):
        def rims(f, _):
            hi, lo = split2(fr[f] * yr[...])
            xrh[f], xrl[f] = hi, lo
            return 0

        lax.fori_loop(0, fields, rims, 0)

        def one_level(l, _):
            columns = pl.ds(pl.multiple_of(l * lat_cells, lat_cells), lat_cells)
            xc = split2((fc[l] * yc[l][None]).reshape(fields * ext, lat_cells))
            xr = (xrh[...].reshape(fields * ext, 2 * lat_cells), xrl[...].reshape(fields * ext, 2 * lat_cells))
            t = dot3(xc, (c_mat[0, l], c_mat[1, l]))
            t = t + dot3(xr, (r_mat[0, :, columns], r_mat[1, :, columns]))
            parts = [
                jnp.concatenate([half[f * ext : (f + 1) * ext] for f in range(fields)], axis=1)
                for half in split2(t)
            ]
            u = dot3((l_mat[0, l], l_mat[1, l]), parts)
            finish(l, [u[:, f * lat_cells : (f + 1) * lat_cells] for f in range(fields)])
            return 0

        lax.fori_loop(0, levels, one_level, 0)

    def finish_cov(l, smoothed):
        acc = fc[l, 0, :lon_cells, :] * smoothed[0]
        for f in range(1, members):
            acc = acc + fc[l, f, :lon_cells, :] * smoothed[f]
        acc = acc * (coef_ens * coef_ens)
        acc = acc + fc[l, members, :lon_cells, :] * smoothed[members] * (coef_static**2 / mem_n)
        part[pl.ds(pl.multiple_of(l * lon_cells, lon_cells), lon_cells), :] = acc

    def piece(owner):
        return pl.ds(pl.multiple_of(owner * chunk, chunk), chunk)

    def mem_copies(src, dst, group):
        out = []
        for j in range(1, mem_n):
            peer = lax.rem(me + j, mem_n)
            copy = pltpu.make_async_remote_copy(
                src_ref=src(peer), dst_ref=dst(j), send_sem=csend.at[group, j],
                recv_sem=crecv.at[group, j], device_id={"mem": peer}, device_id_type=MESH,
            )
            copy.start()
            out.append(copy)
        return out

    def scatter_sum(dst, group):
        copies = mem_copies(lambda peer: part.at[piece(peer)], lambda j: dst.at[j], group)
        acc = part[piece(me), :]
        for j, copy in enumerate(copies):
            copy.wait_recv()
            acc = acc + dst[j + 1]
        for copy in copies:
            copy.wait_send()
        return acc

    def dots_start(left, right, group):
        at = iota((8, lat_cells), 0)
        a = jnp.sum(left, axis=0, keepdims=True)
        b = jnp.sum(right, axis=0, keepdims=True)
        dsend[group] = jnp.where(at == 0, a, jnp.where(at == 1, b, 0.0))
        copies = []
        for step in range(1, total):
            copy = pltpu.make_async_remote_copy(
                src_ref=dsend.at[group], dst_ref=dslots.at[group, step],
                send_sem=dsems.at[group, step], recv_sem=drems.at[group, step],
                device_id=shifted(step), device_id_type=MESH,
            )
            copy.start()
            copies.append(copy)
        return copies

    def dots_end(copies, group):
        for copy in copies:
            copy.wait()
        block = dsend[group] + jnp.sum(dslots[group, 1:], axis=0)
        sums = jnp.sum(block, axis=1, keepdims=True)
        return sums[0:1], sums[1:2]

    apply(bc, br, two_c, two_r, two_l, finish_cov)
    acc = scatter_sum(slots, 0)
    cov[piece(me), :] = acc
    back = mem_copies(lambda peer: cov.at[piece(me)], lambda j: cov.at[piece(me)], 1)
    rhs_mine, diag_mine, cov_mine = bflat[piece(me), :], dflat[piece(me), :], acc
    image_mine = rhs_mine + diag_mine * cov_mine
    dots0 = dots_start(rhs_mine * cov_mine, cov_mine * image_mine, 0)
    for copy in back:
        copy.wait()
    for l in range(levels):
        span = slice(l * lon_cells, (l + 1) * lon_cells)
        qc[l, :lon_cells, :] = bflat[span, :] + dflat[span, :] * cov[span, :]
    lon_q = lon_field(qc, ())
    lon_start(lon_q)
    fill_pack(2, read_q, own, lon_cells)
    lat_q = lat_field(2, qr, (), own)
    lat_q.start()
    lon_wait(lon_q)
    fill_pack(2, read_q, rim, 2 * RIM)
    lat_q2 = lat_field(2, qr, (), rim)
    lat_q2.start()
    lat_q.wait()
    lat_q2.wait()

    apply(qc, qr, two_c, two_r, two_l, finish_cov)
    cov_q = scatter_sum(slots2, 2)
    norm0, curve0 = dots_end(dots0, 0)
    alpha0 = norm0 / curve0
    resid = rhs_mine - alpha0 * image_mine
    cov_r = cov_mine - alpha0 * cov_q
    norm1, curve1 = dots_end(dots_start(resid * cov_r, cov_r * (resid + diag_mine * cov_r), 1), 1)
    beta = norm1 / norm0
    alpha1 = norm1 / (curve1 - beta * norm1 / alpha0)

    def combine(b, q):
        return alpha0 * b + alpha1 * ((b - alpha0 * q) + beta * b)

    for l in range(levels):
        bc[l] = combine(bc[l], qc[l])
    br[...] = combine(br[...], qr[...])

    def finish_control(l, smoothed):
        for f in range(members):
            ens_ref[f, l] = coef_ens * smoothed[f]
        static_ref[l] = coef_static * smoothed[members]

    apply(bc, br, one_c, one_r, one_l, finish_control)


def per_device(anomalies, spread, obs_index, innovation, obs_weight, band_width):
    members = anomalies.shape[0]
    levels, lon_cells, lat_cells = spread.shape
    sizes = tuple(lax.axis_size(a) for a in AXES)
    mem_n, total = sizes[2], math.prod(sizes)
    fields = members + 1
    ext = lon_cells + 2 * RIM
    rows = levels * lon_cells
    chunk = rows // mem_n
    v = pltpu.VMEM
    sem = pltpu.SemaphoreType.DMA
    edge = v((members, levels * RIM, lat_cells), BF16)
    packed = v((members, ext, lat_cells), BF16)
    field = v((levels, ext, lat_cells), F32)
    field_rim = v((ext, 2 * lat_cells), F32)
    mats = [
        v((2, levels, lat_cells, lat_cells), BF16),
        v((2, 2 * lat_cells, levels * lat_cells), BF16),
        v((2, levels, lon_cells, ext), BF16),
    ]
    flat = v((rows, lat_cells), F32)
    scratch = [
        v((levels, fields, ext, lat_cells), F32),
        v((fields, ext, 2 * lat_cells), F32),
        field, field_rim, field, field_rim,
        edge, edge, edge, edge,
        packed, packed, packed, packed,
        v((3, 2, ext, lat_cells), F32),
        v((fields, ext, 2 * lat_cells), BF16),
        v((fields, ext, 2 * lat_cells), BF16),
        *mats, *mats,
        flat, flat, flat, flat,
        v((mem_n, chunk, lat_cells), F32),
        v((mem_n, chunk, lat_cells), F32),
        v((2, total, 8, lat_cells), F32),
        v((2, 8, lat_cells), F32),
        sem((32,)), sem((32,)), sem((3, mem_n)), sem((3, mem_n)), sem((2, total)), sem((2, total)),
    ]
    kernel = functools.partial(fused, dims=(members, levels, lon_cells, lat_cells, sizes))
    return pl.pallas_call(
        kernel,
        out_shape=[
            jax.ShapeDtypeStruct((members, levels, lon_cells, lat_cells), F32),
            jax.ShapeDtypeStruct((levels, lon_cells, lat_cells), F32),
        ],
        in_specs=[VMEM] * 5 + [pl.BlockSpec(memory_space=pltpu.SMEM)],
        out_specs=[VMEM] * 2,
        scratch_shapes=scratch,
        compiler_params=pltpu.CompilerParams(
            collective_id=0, has_side_effects=True, vmem_limit_bytes=60 * 2**20
        ),
    )(
        anomalies, spread, obs_index.reshape(1, -1), obs_weight.reshape(1, -1),
        innovation.reshape(1, -1), band_width,
    )


def solution(mesh):
    return jax.shard_map(
        per_device,
        mesh=mesh,
        in_specs=(
            P("mem", None, "lon", "lat"),
            P(None, "lon", "lat"),
            P("lon", "lat", None),
            P("lon", "lat", None),
            P("lon", "lat", None),
            P(),
        ),
        out_specs=(P("mem", None, "lon", "lat"), P(None, "lon", "lat")),
        check_vma=False,
    )
```

```python
import functools
import math

import jax
import jax.numpy as jnp
from jax import lax
from jax.experimental import pallas as pl
from jax.experimental.pallas import tpu as pltpu
from jax.sharding import PartitionSpec as P

BAND = 12
RIM = 2 * BAND

hybrid_ens = 0.75
hybrid_static = 0.25

MESH = pl.DeviceIdType.MESH
VMEM = pl.BlockSpec(memory_space=pltpu.VMEM)
F32 = jnp.float32
BF16 = jnp.bfloat16


def split2(x):
    hi = x.astype(BF16)
    return hi, (x - hi.astype(F32)).astype(BF16)


def dot3(left, right):
    lh, ll = left
    rh, rl = right
    d = functools.partial(jnp.dot, preferred_element_type=F32)
    return d(lh, rh) + (d(ll, rh) + d(lh, rl))


AXES = ("lon", "lat", "mem")


def fused(a_ref, s_ref, i_ref, w_ref, v_ref, bw_ref, ens_ref, static_ref, *scratch, dims):
    members, levels, lon_cells, lat_cells, sizes = dims
    (fc, fr, bc, br, qc, qr, send_al, send_ah, recv_al, recv_ah, pack_l, pack_h, recv_pl, recv_ph,
     fpack, xrh, xrl, two_c, two_r, two_l, one_c, one_r, one_l, bflat, dflat, cov, part,
     slots, slots2, dslots, dsend, smoothed_lat, send, recv, csend, crecv, dsems, drems) = scratch
    lon_n, lat_n, mem_n = sizes
    total = lon_n * lat_n * mem_n
    fields = members + 1
    ext = lon_cells + 2 * RIM
    rows = levels * lon_cells
    chunk = rows // mem_n
    coef_ens = math.sqrt(hybrid_ens / (members * mem_n))
    coef_static = math.sqrt(hybrid_static)
    mine = [lax.axis_index(a) for a in AXES]
    lat_at, me = mine[1], mine[2]
    has_low, has_high = lat_at > 0, lat_at < lat_n - 1

    def shifted(step):
        parts, rest = [], step
        for size in reversed(sizes):
            parts.append(rest % size)
            rest //= size
        return tuple(lax.rem(m + s, size) for m, s, size in zip(mine, reversed(parts), sizes))

    barrier = pltpu.get_barrier_semaphore()
    for step in range(1, total):
        pl.semaphore_signal(barrier, inc=1, device_id=shifted(step), device_id_type=MESH)

    used = [0]

    def remote(src, dst, where):
        k = used[0]
        used[0] += 1
        return pltpu.make_async_remote_copy(
            src_ref=src, dst_ref=dst, send_sem=send.at[k], recv_sem=recv.at[k],
            device_id=where, device_id_type=MESH,
        )

    lon_low = {"lon": lax.rem(mine[0] + lon_n - 1, lon_n)}
    lon_high = {"lon": lax.rem(mine[0] + 1, lon_n)}
    lat_low = {"lat": lax.rem(lat_at + lat_n - 1, lat_n)}
    lat_high = {"lat": lax.rem(lat_at + 1, lat_n)}
    own = pl.ds(0, lon_cells)
    rim = pl.ds(lon_cells, 2 * RIM)
    low_rows = pl.ds(lon_cells, RIM)
    high_rows = pl.ds(lon_cells + RIM, RIM)
    first_rows = pl.ds(0, RIM)
    last_rows = pl.ds(lon_cells - RIM, RIM)
    low_lanes = pl.ds(0, lat_cells)
    high_lanes = pl.ds(lat_cells, lat_cells)

    def lon_start(copies):
        for c in copies:
            c.start()

    def lon_wait(copies):
        for c in copies:
            c.wait()

    class Lat:
        def __init__(self, low_src, high_src, from_low, from_high):
            self.to_low = remote(low_src, from_high, lat_low)
            self.to_high = remote(high_src, from_low, lat_high)

        def start(self):
            pl.when(has_low)(self.to_low.start)
            pl.when(has_high)(self.to_high.start)

        def wait(self):
            pl.when(has_low)(self.to_low.wait_send)
            pl.when(has_high)(self.to_high.wait_send)
            pl.when(has_high)(self.to_low.wait_recv)
            pl.when(has_low)(self.to_high.wait_recv)

    def lane_pack(read, count):
        lane = lax.broadcasted_iota(jnp.int32, (count, lat_cells), 1)
        low = jnp.zeros((count, lat_cells), F32)
        high = low
        for l in range(levels):
            x = read(l)
            here = (lane >= l * RIM) & (lane < (l + 1) * RIM)
            low = jnp.where(here, pltpu.roll(x, (l * RIM) % lat_cells, 1), low)
            high = jnp.where(here, pltpu.roll(x, ((l + 1) * RIM) % lat_cells, 1), high)
        return low, high

    def zero_edges(ref, lead=()):
        @pl.when(jnp.logical_not(has_low))
        def _():
            ref[(*lead, slice(None), low_lanes)] = jnp.zeros((ext, lat_cells), F32)

        @pl.when(jnp.logical_not(has_high))
        def _():
            ref[(*lead, slice(None), high_lanes)] = jnp.zeros((ext, lat_cells), F32)

    def load_member(m, _):
        lows, highs = [], []
        for l in range(levels):
            x = a_ref[m, l].astype(F32)
            fc[l, m, :lon_cells, :] = x
            lows.append(x[:RIM])
            highs.append(x[lon_cells - RIM :])
        send_al[m] = jnp.concatenate(lows, axis=0).astype(BF16)
        send_ah[m] = jnp.concatenate(highs, axis=0).astype(BF16)
        return 0

    lax.fori_loop(0, members, load_member, 0)
    for l in range(levels):
        fc[l, members, :lon_cells, :] = s_ref[l]

    def pack_member(span, count):
        def go(m, _):
            low, high = lane_pack(lambda l: fc[l, m, span, :], count)
            pack_l[m, span, :] = low.astype(BF16)
            pack_h[m, span, :] = high.astype(BF16)
            return 0

        lax.fori_loop(0, members, go, 0)

    def lon_field(ref, lead):
        at = lambda span: ref.at[(slice(None), *lead, span, slice(None))]
        return [
            remote(at(first_rows), at(high_rows), lon_low),
            remote(at(last_rows), at(low_rows), lon_high),
        ]

    def lat_field(slot, dst, lead, span):
        at = lambda lanes: dst.at[(*lead, span, lanes)]
        return Lat(
            fpack.at[slot, 0, span, :], fpack.at[slot, 1, span, :], at(low_lanes), at(high_lanes)
        )

    def fill_pack(slot, read, span, count):
        low, high = lane_pack(lambda l: read(l, span), count)
        fpack[slot, 0, span, :] = low
        fpack[slot, 1, span, :] = high

    read_s = lambda l, span: fc[l, members, span, :]
    read_b = lambda l, span: bc[l, span, :]
    read_q = lambda l, span: qc[l, span, :]

    pl.semaphore_wait(barrier, total - 1)
    lon_a = [remote(send_al, recv_ah, lon_low), remote(send_ah, recv_al, lon_high)]
    lon_start(lon_a)
    lon_s = lon_field(fc, (members,))
    lon_start(lon_s)
    pack_member(own, lon_cells)
    lat_a = Lat(pack_l.at[:, own, :], pack_h.at[:, own, :], recv_pl.at[:, own, :], recv_ph.at[:, own, :])
    lat_a.start()

    idx, val_w = i_ref[...], w_ref[...]
    n_obs = idx.shape[1]
    row, lane = idx // lat_cells, idx % lat_cells
    at_row = (lax.broadcasted_iota(jnp.int32, (rows, n_obs), 0) == row).astype(F32).astype(BF16)
    at_lane = lax.broadcasted_iota(jnp.int32, (lat_cells, n_obs), 0) == lane
    for val, out in ((val_w, dflat), (val_w * v_ref[...], bflat)):
        acc = None
        for _ in range(3):
            piece_val = val.astype(BF16).astype(F32)
            val = val - piece_val
            placed = jnp.where(at_lane, piece_val, 0.0).astype(BF16)
            term = lax.dot_general(
                at_row, placed, (((1,), (1,)), ((), ())), preferred_element_type=F32
            )
            acc = term if acc is None else acc + term
        out[...] = acc
    for l in range(levels):
        bc[l, :lon_cells, :] = bflat[l * lon_cells : (l + 1) * lon_cells, :]
    lon_b = lon_field(bc, ())
    lon_start(lon_b)
    fill_pack(0, read_s, own, lon_cells)
    fill_pack(1, read_b, own, lon_cells)
    lat_sb = [lat_field(0, fr, (members,), own), lat_field(1, br, (), own)]
    for c in lat_sb:
        c.start()
    zero_edges(fr, (members,))
    zero_edges(br)
    zero_edges(qr)

    def iota(shape, dim):
        return lax.broadcasted_iota(jnp.int32, shape, dim)

    def ext_place(index, cells):
        return jnp.where(index < cells, index, jnp.where(index < cells + RIM, index - cells - RIM, index - RIM))

    def make_matrices(l, _):
        taps = (iota((8, 128), 1) - BAND).astype(F32)

        def weights(kind):
            width = bw_ref[kind, l].astype(F32) + jnp.zeros((1, 1), F32)

            def raw(o):
                return jnp.where(jnp.abs(o) <= width, jnp.exp(-0.5 * (o / (0.5 * width)) ** 2), 0.0)

            norm = jnp.sum(raw(taps)[:1], axis=1, keepdims=True)
            return lambda o: raw(o.astype(F32)) / norm

        def put(ref, where, value):
            hi, lo = split2(value)
            ref[(0, *where)] = hi
            ref[(1, *where)] = lo

        w = weights(0)
        mids = 128 * pl.cdiv(lon_cells + 2 * BAND, 128)
        near = w(iota((lon_cells, mids), 0) - (iota((lon_cells, mids), 1) - BAND))
        near = jnp.where(iota((lon_cells, mids), 1) < lon_cells + 2 * BAND, near, 0.0)
        far = w(iota((mids, ext), 0) - BAND - ext_place(iota((mids, ext), 1), lon_cells))
        put(two_l, (l,), dot3(split2(near), split2(far)))
        put(one_l, (l,), w(iota((lon_cells, ext), 0) - ext_place(iota((lon_cells, ext), 1), lon_cells)))

        w = weights(1)
        mids = 128 * pl.cdiv(lat_cells + 2 * BAND, 128)
        mid = iota((mids, lat_cells), 0) - BAND
        place = lat_at * lat_cells + mid
        keep = (place >= 0) & (place < lat_cells * lat_n) & (mid < lat_cells + BAND)
        back = split2(jnp.where(keep, w(mid - iota((mids, lat_cells), 1)), 0.0))
        out = iota((lat_cells, lat_cells), 1)
        here = iota((lat_cells, mids), 0) - (iota((lat_cells, mids), 1) - BAND)
        put(two_c, (l,), dot3(split2(w(here)), back))
        put(one_c, (l,), w(iota((lat_cells, lat_cells), 0) - out))
        columns = pl.ds(pl.multiple_of(l * lat_cells, lat_cells), lat_cells)
        for side in range(2):
            shift = -RIM if side == 0 else lat_cells
            span = pl.ds(side * lat_cells, lat_cells)

            def rim_at(shape):
                p = iota(shape, 0) - l * RIM
                return p + shift, (p >= 0) & (p < RIM)

            pos, ok = rim_at((lat_cells, mids))
            there = jnp.where(ok, w(pos - (iota((lat_cells, mids), 1) - BAND)), 0.0)
            put(two_r, (span, columns), dot3(split2(there), back))
            pos, ok = rim_at((lat_cells, lat_cells))
            put(one_r, (span, columns), jnp.where(ok, w(pos - out), 0.0))
        return 0

    lax.fori_loop(0, levels, make_matrices, 0)

    def lat_part(yc, yr, c_mat, r_mat, l, span, count):
        columns = pl.ds(pl.multiple_of(l * lat_cells, lat_cells), lat_cells)
        xc = split2((fc[l, :, span, :] * yc[l, span, :][None]).reshape(fields * count, lat_cells))
        xr = (
            xrh[:, span, :].reshape(fields * count, 2 * lat_cells),
            xrl[:, span, :].reshape(fields * count, 2 * lat_cells),
        )
        t = dot3(xc, (c_mat[0, l], c_mat[1, l]))
        t = t + dot3(xr, (r_mat[0, :, columns], r_mat[1, :, columns]))
        for h, half in enumerate(split2(t)):
            smoothed_lat[h, l, span, :] = jnp.concatenate(
                [half[f * count : (f + 1) * count] for f in range(fields)], axis=1
            )

    def rim_products(yr, span):
        def go(f, _):
            hi, lo = split2(fr[f, span, :] * yr[span, :])
            xrh[f, span, :], xrl[f, span, :] = hi, lo
            return 0

        lax.fori_loop(0, fields, go, 0)

    def apply_own(yc, yr, mats):
        rim_products(yr, own)

        def go(l, _):
            lat_part(yc, yr, mats[0], mats[1], l, own, lon_cells)
            return 0

        lax.fori_loop(0, levels, go, 0)

    def apply_rim(yc, yr, mats, finish):
        rim_products(yr, rim)

        def go(i, _):
            l = lax.rem(me + 1 + i, levels)
            lat_part(yc, yr, mats[0], mats[1], l, rim, 2 * RIM)
            u = dot3((mats[2][0, l], mats[2][1, l]), (smoothed_lat[0, l], smoothed_lat[1, l]))
            finish(i, l, [u[:, f * lat_cells : (f + 1) * lat_cells] for f in range(fields)])
            return 0

        lax.fori_loop(0, levels, go, 0)

    def unpack_lat(span, count):
        for ref, keep, lanes in ((recv_pl, has_low, low_lanes), (recv_ph, has_high, high_lanes)):
            def go(m, _):
                fr[m, span, lanes] = ref[m, span, :].astype(F32)
                return 0

            def clear(m, _):
                fr[m, span, lanes] = jnp.zeros((count, lat_cells), F32)
                return 0

            @pl.when(keep)
            def _():
                lax.fori_loop(0, members, go, 0)

            @pl.when(jnp.logical_not(keep))
            def _():
                lax.fori_loop(0, members, clear, 0)

    lat_a.wait()
    unpack_lat(own, lon_cells)
    for c in lat_sb:
        c.wait()
    apply_own(bc, br, (two_c, two_r, two_l))

    lon_wait(lon_a)

    def unpack_member(m, _):
        low, high = recv_al[m].astype(F32), recv_ah[m].astype(F32)
        for l in range(levels):
            fc[l, m, low_rows, :] = low[l * RIM : (l + 1) * RIM]
            fc[l, m, high_rows, :] = high[l * RIM : (l + 1) * RIM]
        return 0

    lax.fori_loop(0, members, unpack_member, 0)
    pack_member(rim, 2 * RIM)
    lat_a2 = Lat(pack_l.at[:, rim, :], pack_h.at[:, rim, :], recv_pl.at[:, rim, :], recv_ph.at[:, rim, :])
    lat_a2.start()
    lon_wait(lon_s)
    lon_wait(lon_b)
    fill_pack(0, read_s, rim, 2 * RIM)
    fill_pack(1, read_b, rim, 2 * RIM)
    lat_sb2 = [lat_field(0, fr, (members,), rim), lat_field(1, br, (), rim)]
    for c in lat_sb2:
        c.start()
    lat_a2.wait()
    unpack_lat(rim, 2 * RIM)
    for c in lat_sb2:
        c.wait()

    def piece(owner):
        return pl.ds(pl.multiple_of(owner * chunk, chunk), chunk)

    def mem_copy(src, dst, j, group):
        return pltpu.make_async_remote_copy(
            src_ref=src, dst_ref=dst, send_sem=csend.at[group, j], recv_sem=crecv.at[group, j],
            device_id={"mem": lax.rem(me + j, mem_n)}, device_id_type=MESH,
        )

    def sum_copy(dst, j, group):
        return mem_copy(part.at[piece(lax.rem(me + j, mem_n))], dst.at[j], j, group)

    by_level = levels == mem_n

    def finish_cov(dst, group):
        def finish(i, l, smoothed):
            acc = fc[l, 0, :lon_cells, :] * smoothed[0]
            for f in range(1, members):
                acc = acc + fc[l, f, :lon_cells, :] * smoothed[f]
            acc = acc * (coef_ens * coef_ens)
            acc = acc + fc[l, members, :lon_cells, :] * smoothed[members] * (coef_static**2 / mem_n)
            part[pl.ds(pl.multiple_of(l * lon_cells, lon_cells), lon_cells), :] = acc
            if by_level:
                @pl.when(i < mem_n - 1)
                def _():
                    sum_copy(dst, i + 1, group).start()

        return finish

    def scatter_sum(dst, group):
        copies = [sum_copy(dst, j, group) for j in range(1, mem_n)]
        if not by_level:
            for copy in copies:
                copy.start()
        acc = part[piece(me), :]
        for j, copy in enumerate(copies):
            copy.wait_recv()
            acc = acc + dst[j + 1]
        for copy in copies:
            copy.wait_send()
        return acc

    def dots_start(left, right, group):
        at = iota((2, lat_cells), 0)
        a = jnp.sum(left, axis=0, keepdims=True)
        b = jnp.sum(right, axis=0, keepdims=True)
        dsend[group] = jnp.where(at == 0, a, b)
        copies = []
        for step in range(1, total):
            copy = pltpu.make_async_remote_copy(
                src_ref=dsend.at[group], dst_ref=dslots.at[group, step],
                send_sem=dsems.at[group, step], recv_sem=drems.at[group, step],
                device_id=shifted(step), device_id_type=MESH,
            )
            copy.start()
            copies.append(copy)
        return copies

    def dots_end(copies, group):
        for copy in copies:
            copy.wait()
        block = dsend[group] + jnp.sum(dslots[group, 1:], axis=0)
        sums = jnp.sum(block, axis=1, keepdims=True)
        return sums[0:1], sums[1:2]

    two, one = (two_c, two_r, two_l), (one_c, one_r, one_l)
    apply_rim(bc, br, two, finish_cov(slots, 0))
    acc = scatter_sum(slots, 0)
    cov[piece(me), :] = acc
    back = [mem_copy(cov.at[piece(me)], cov.at[piece(me)], j, 1) for j in range(1, mem_n)]
    for copy in back:
        copy.start()
    rhs_mine, diag_mine, cov_mine = bflat[piece(me), :], dflat[piece(me), :], acc
    image_mine = rhs_mine + diag_mine * cov_mine
    dots0 = dots_start(rhs_mine * cov_mine, cov_mine * image_mine, 0)
    for copy in back:
        copy.wait()
    for l in range(levels):
        span = slice(l * lon_cells, (l + 1) * lon_cells)
        qc[l, :lon_cells, :] = bflat[span, :] + dflat[span, :] * cov[span, :]
    lon_q = lon_field(qc, ())
    lon_start(lon_q)
    fill_pack(2, read_q, own, lon_cells)
    lat_q = lat_field(2, qr, (), own)
    lat_q.start()
    lon_wait(lon_q)
    fill_pack(2, read_q, rim, 2 * RIM)
    lat_q2 = lat_field(2, qr, (), rim)
    lat_q2.start()
    lat_q.wait()

    apply_own(qc, qr, two)
    lat_q2.wait()
    apply_rim(qc, qr, two, finish_cov(slots2, 2))
    cov_q = scatter_sum(slots2, 2)
    norm0, curve0 = dots_end(dots0, 0)
    alpha0 = norm0 / curve0
    resid = rhs_mine - alpha0 * image_mine
    cov_r = cov_mine - alpha0 * cov_q
    norm1, curve1 = dots_end(dots_start(resid * cov_r, cov_r * (resid + diag_mine * cov_r), 1), 1)
    beta = norm1 / norm0
    alpha1 = norm1 / (curve1 - beta * norm1 / alpha0)

    def combine(b, q):
        return alpha0 * b + alpha1 * ((b - alpha0 * q) + beta * b)

    for l in range(levels):
        bc[l] = combine(bc[l], qc[l])
    br[...] = combine(br[...], qr[...])

    def finish_control(i, l, smoothed):
        for f in range(members):
            ens_ref[f, l] = coef_ens * smoothed[f]
        static_ref[l] = coef_static * smoothed[members]

    apply_own(bc, br, one)
    apply_rim(bc, br, one, finish_control)


def per_device(anomalies, spread, obs_index, innovation, obs_weight, band_width):
    members = anomalies.shape[0]
    levels, lon_cells, lat_cells = spread.shape
    sizes = tuple(lax.axis_size(a) for a in AXES)
    mem_n, total = sizes[2], math.prod(sizes)
    fields = members + 1
    ext = lon_cells + 2 * RIM
    rows = levels * lon_cells
    chunk = rows // mem_n
    v = pltpu.VMEM
    sem = pltpu.SemaphoreType.DMA
    edge = v((members, levels * RIM, lat_cells), BF16)
    packed = v((members, ext, lat_cells), BF16)
    field = v((levels, ext, lat_cells), F32)
    field_rim = v((ext, 2 * lat_cells), F32)
    mats = [
        v((2, levels, lat_cells, lat_cells), BF16),
        v((2, 2 * lat_cells, levels * lat_cells), BF16),
        v((2, levels, lon_cells, ext), BF16),
    ]
    flat = v((rows, lat_cells), F32)
    scratch = [
        v((levels, fields, ext, lat_cells), F32),
        v((fields, ext, 2 * lat_cells), F32),
        field, field_rim, field, field_rim,
        edge, edge, edge, edge,
        packed, packed, packed, packed,
        v((3, 2, ext, lat_cells), F32),
        v((fields, ext, 2 * lat_cells), BF16),
        v((fields, ext, 2 * lat_cells), BF16),
        *mats, *mats,
        flat, flat, flat, flat,
        v((mem_n, chunk, lat_cells), F32),
        v((mem_n, chunk, lat_cells), F32),
        v((2, total, 2, lat_cells), F32),
        v((2, 2, lat_cells), F32),
        v((2, levels, ext, fields * lat_cells), BF16),
        sem((32,)), sem((32,)), sem((3, mem_n)), sem((3, mem_n)), sem((2, total)), sem((2, total)),
    ]
    kernel = functools.partial(fused, dims=(members, levels, lon_cells, lat_cells, sizes))
    return pl.pallas_call(
        kernel,
        out_shape=[
            jax.ShapeDtypeStruct((members, levels, lon_cells, lat_cells), F32),
            jax.ShapeDtypeStruct((levels, lon_cells, lat_cells), F32),
        ],
        in_specs=[VMEM] * 5 + [pl.BlockSpec(memory_space=pltpu.SMEM)],
        out_specs=[VMEM] * 2,
        scratch_shapes=scratch,
        compiler_params=pltpu.CompilerParams(
            collective_id=0, has_side_effects=True, vmem_limit_bytes=60 * 2**20
        ),
    )(
        anomalies, spread, obs_index.reshape(1, -1), obs_weight.reshape(1, -1),
        innovation.reshape(1, -1), band_width,
    )


def solution(mesh):
    return jax.shard_map(
        per_device,
        mesh=mesh,
        in_specs=(
            P("mem", None, "lon", "lat"),
            P(None, "lon", "lat"),
            P("lon", "lat", None),
            P("lon", "lat", None),
            P("lon", "lat", None),
            P(),
        ),
        out_specs=(P("mem", None, "lon", "lat"), P(None, "lon", "lat")),
        check_vma=False,
    )
```
